32 devices in a mesh: dp: 2 (over z, core), tp: 16 (over x, y).
Axes of the slice: x: 4, y: 4, z: 1, core: 2. Of those that a mesh axis runs over, the one named last changes fastest.
The devices are a block of a 4x4x8 slice.
Arguments:
- x: bfloat16 [4096, 7168], P('dp'), parts along dimension 0
- w_gate: bfloat16 [7168, 18432], P(None, 'tp')
- w_up: bfloat16 [7168, 18432], P(None, 'tp')
- w_down: bfloat16 [18432, 7168], P('tp')
Outputs:
- output: bfloat16 [4096, 7168], P('dp'), parts along dimension 0
There are 2 independent parts. The reference program is written for one: setup_inputs(seed, part) draws one part's arguments, and reference() takes and returns one part's arrays. A program takes and returns all parts, laid end to end along the dimension named above; an argument that names none is the same for every part.
All inputs are finite; a program needn't handle non-finite values.
Results may differ from the reference program's by a relative error of at most 0.016.
Values are sent between devices in bfloat16 or wider.
A program may use at most 768 MiB of HBM per device.

```python
import jax
import jax.numpy as jnp

ROWS = 2048
D = 7168
FF = 18432


def setup_inputs(seed: int = 0, part: int = 0) -> dict:
    kx, kg, ku, kd = jax.random.split(jax.random.key(seed), 4)
    drawn = {
        "x": jax.random.normal(jax.random.fold_in(kx, part), (ROWS, D), jnp.float32),
        "w_gate": jax.random.normal(kg, (D, FF), jnp.float32) * D**-0.5,
        "w_up": jax.random.normal(ku, (D, FF), jnp.float32) * D**-0.5,
        "w_down": jax.random.normal(kd, (FF, D), jnp.float32) * FF**-0.5,
    }
    return {k: v.astype(jnp.bfloat16) for k, v in drawn.items()}


def reference(x, w_gate, w_up, w_down):
    gate = jnp.dot(x, w_gate, preferred_element_type=jnp.float32)
    up = jnp.dot(x, w_up, preferred_element_type=jnp.float32)
    hidden = (jax.nn.silu(gate) * up).astype(jnp.bfloat16)
    return jnp.dot(hidden, w_down, preferred_element_type=jnp.float32).astype(jnp.bfloat16)
```

```python
import functools
import math

import jax
import jax.numpy as jnp
from jax import lax
from jax.experimental import pallas as pl
from jax.experimental.pallas import tpu as pltpu
from jax.sharding import PartitionSpec as P

F32 = jnp.float32
BF16 = jnp.bfloat16

CHUNK = 256
STREAMS = 8
TILE = 128
GU_SLOTS = 3
DN_SLOTS = 3


def kernel(
    side,
    x_hbm, wg_hbm, wu_hbm, wd_hbm, y_hbm,
    x_buf, gu_buf, dn_buf, hidden, part, xred, out1, in1, out2, in2, fin,
    x_sem, gu_sem, dn_sem, fin_sem,
    send1, recv1, send2, recv2, send3, recv3, send4, recv4,
):
    rows, depth = x_hbm.shape
    width = wd_hbm.shape[1] // STREAMS
    ff = wg_hbm.shape[1]
    chunks = rows // CHUNK
    piece = CHUNK // side
    sub = piece // side
    steps = side - 1
    gu_units = ff // TILE
    units = gu_units + STREAMS
    slots = steps * 8

    me = lax.axis_index("tp")
    px, py = me // side, me % side

    def place(stream):
        colour = stream % 4
        first_x = 1 - colour // 2
        d = 1 - 2 * (colour % 2)
        along_x = ((px + d + side) % side) * side + py
        along_y = px * side + (py + d + side) % side
        p1 = first_x * px + (1 - first_x) * py
        p2 = first_x * py + (1 - first_x) * px
        n1 = first_x * along_x + (1 - first_x) * along_y
        n2 = first_x * along_y + (1 - first_x) * along_x
        return d, p1, p2, n1, n2

    def cols(stream):
        return pl.ds(pl.multiple_of(stream * width, 128), width)

    def y_rows(start, size):
        return pl.ds(pl.multiple_of(start, 16), size)

    def x_copy(j):
        return pltpu.make_async_copy(
            x_hbm.at[pl.ds(pl.multiple_of(j * CHUNK, CHUNK), CHUNK)], x_buf.at[j % 2], x_sem.at[j % 2]
        )

    def gu_copies(g):
        src = pl.ds(pl.multiple_of((g % gu_units) * TILE, TILE), TILE)
        slot = g % GU_SLOTS
        return (
            pltpu.make_async_copy(wg_hbm.at[:, src], gu_buf.at[slot, :, pl.ds(0, TILE)], gu_sem.at[slot, 0]),
            pltpu.make_async_copy(wu_hbm.at[:, src], gu_buf.at[slot, :, pl.ds(TILE, TILE)], gu_sem.at[slot, 1]),
        )

    def dn_copy(g):
        slot = g % DN_SLOTS
        return pltpu.make_async_copy(wd_hbm.at[:, cols(g % STREAMS)], dn_buf.at[slot], dn_sem.at[slot])

    def unit(j, u):
        @pl.when(u < gu_units)
        def _():
            g = j * gu_units + u

            @pl.when(u == 0)
            def _():
                x_copy(j).wait()

            for c in gu_copies(g):
                c.wait()
            both = jnp.dot(x_buf[j % 2], gu_buf[g % GU_SLOTS], preferred_element_type=F32)
            gate, up = both[:, :TILE], both[:, TILE:]
            hidden[u] = (jax.nn.silu(gate) * up).astype(BF16)

            @pl.when(g + GU_SLOTS < chunks * gu_units)
            def _():
                for c in gu_copies(g + GU_SLOTS):
                    c.start()

            @pl.when((u == gu_units - 1) & (j + 2 < chunks))
            def _():
                x_copy(j + 2).start()

        @pl.when(u >= gu_units)
        def _():
            s = u - gu_units
            g = j * STREAMS + s
            dn_copy(g).wait()
            h = jnp.concatenate([hidden[i] for i in range(gu_units)], axis=1)
            part[j % 2, s] = jnp.dot(h, dn_buf[g % DN_SLOTS], preferred_element_type=F32)

            @pl.when(g + DN_SLOTS < chunks * STREAMS)
            def _():
                dn_copy(g + DN_SLOTS).start()

    def remote(src, dst, ssem, rsem, to):
        return pltpu.make_async_remote_copy(
            src_ref=src, dst_ref=dst, send_sem=ssem, recv_sem=rsem,
            device_id={"tp": to}, device_id_type=pl.DeviceIdType.MESH,
        )

    def rs1(j, k, s):
        _, _, _, n1, _ = place(s)
        return remote(out1.at[k, s], in1.at[j % 2, k, s], send1.at[k, s], recv1.at[j % 2, k, s], n1)

    def rs2(j, k, s):
        _, _, _, _, n2 = place(s)
        return remote(out2.at[k, s], in2.at[j % 2, k, s], send2.at[k, s], recv2.at[j % 2, k, s], n2)

    def ag2(j, k, s, own):
        d, p1, p2, _, n2 = place(s)
        r = (p2 - d * k + 2 * side) % side
        at = y_hbm.at[y_rows(j * CHUNK + p1 * piece + r * sub, sub), cols(s)]
        return remote(fin.at[s] if own else at, at, send3.at[k, s], recv3.at[j % 2, k, s], n2)

    def ag1(j, k, s):
        d, p1, _, n1, _ = place(s)
        q = (p1 - d * k + 2 * side) % side
        at = y_hbm.at[y_rows(j * CHUNK + q * piece, piece), cols(s)]
        return remote(at, at, send4.at[k, s], recv4.at[j % 2, k, s], n1)

    def fin_copy(j, s):
        _, p1, p2, _, _ = place(s)
        at = y_hbm.at[y_rows(j * CHUNK + p1 * piece + p2 * sub, sub), cols(s)]
        return pltpu.make_async_copy(fin.at[s], at, fin_sem.at[s])

    def each(half, f):
        lax.fori_loop(0, 4, lambda c, _: (f(half * 4 + c), 0)[1], 0)

    def phase1(j, k, half):
        def add(s):
            d, p1, _, _, _ = place(s)
            q = (p1 - d * (1 + k) + 2 * side) % side
            mine = part[j % 2, s, pl.ds(pl.multiple_of(q * piece, piece), piece), :]

            @pl.when(j > 0)
            def _():
                rs1(j - 1, k, s).wait_send()

            @pl.when(k == 0)
            def _():
                out1[0, s] = mine.astype(BF16)

            @pl.when(k > 0)
            def _():
                rs1(j, k - 1, s).wait_recv()
                out1[k, s] = (mine + in1[j % 2, k - 1, s].astype(F32)).astype(BF16)

        each(half, add)
        each(half, lambda s: rs1(j, k, s).start())

    def phase2(j, k, half):
        def add(s):
            d, p1, p2, _, _ = place(s)
            r = (p2 - d * (1 + k) + 2 * side) % side
            at = pl.ds(pl.multiple_of(r * sub, sub), sub)

            @pl.when(j > 0)
            def _():
                rs2(j - 1, k, s).wait_send()

            @pl.when(k == 0)
            def _():
                rs1(j, steps - 1, s).wait_recv()
                mine = part[j % 2, s, pl.ds(pl.multiple_of(p1 * piece, piece), piece), :]
                xred[j % 2, s] = mine + in1[j % 2, steps - 1, s].astype(F32)
                out2[0, s] = xred[j % 2, s, at, :].astype(BF16)

            @pl.when(k > 0)
            def _():
                rs2(j, k - 1, s).wait_recv()
                out2[k, s] = (xred[j % 2, s, at, :] + in2[j % 2, k - 1, s].astype(F32)).astype(BF16)

        each(half, add)
        each(half, lambda s: rs2(j, k, s).start())

    def phase3(j, k, half):
        @pl.when(k == 0)
        def _():
            def add(s):
                _, _, p2, _, _ = place(s)

                @pl.when(j > 0)
                def _():
                    ag2(j - 1, 0, s, True).wait_send()

                rs2(j, steps - 1, s).wait_recv()
                mine = xred[j % 2, s, pl.ds(pl.multiple_of(p2 * sub, sub), sub), :]
                fin[s] = (mine + in2[j % 2, steps - 1, s].astype(F32)).astype(BF16)

            def go(s):
                ag2(j, 0, s, True).start()
                fin_copy(j, s).start()

            each(half, add)
            each(half, go)

        @pl.when(k > 0)
        def _():
            def go(s):
                @pl.when(j > 0)
                def _():
                    ag2(j - 1, k, s, False).wait_send()

                @pl.when(k == 1)
                def _():
                    fin_copy(j, s).wait()

                ag2(j, k - 1, s, False).wait_recv()
                ag2(j, k, s, False).start()

            each(half, go)

    def phase4(j, k, half):
        def go(s):
            @pl.when(j > 0)
            def _():
                ag1(j - 1, k, s).wait_send()

            @pl.when(k == 0)
            def _():
                ag2(j, steps - 1, s, False).wait_recv()

                @pl.when(j > 0)
                def _():
                    ag1(j - 1, steps - 1, s).wait_recv()

            @pl.when(k > 0)
            def _():
                ag1(j, k - 1, s).wait_recv()

            ag1(j, k, s).start()

        each(half, go)

    x_copy(0).start()
    for g in range(GU_SLOTS):
        for c in gu_copies(g):
            c.start()
    for g in range(DN_SLOTS):
        dn_copy(g).start()
    x_copy(1).start()

    barrier = pltpu.get_barrier_semaphore()
    for to in (
        ((px + 1) % side) * side + py,
        ((px + side - 1) % side) * side + py,
        px * side + (py + 1) % side,
        px * side + (py + side - 1) % side,
    ):
        pl.semaphore_signal(barrier, inc=1, device_id={"tp": to}, device_id_type=pl.DeviceIdType.MESH)
    pl.semaphore_wait(barrier, 4)

    def slot(n, carry):
        filling = n < units
        i = jnp.where(filling, 0, n - units)
        t, rest = i // slots, i % slots
        k, m = rest // 8, rest % 8
        half = m % 2
        for phase, f in enumerate((phase1, phase2, phase3, phase4)):
            @pl.when((n >= units) & (m // 2 == phase) & (t >= phase) & (t - phase < chunks))
            def _():
                f(t - phase, k, half)

        u = jnp.where(filling, n, (units * rest) // slots)
        busy = filling | ((units * (rest + 1)) // slots > (units * rest) // slots)
        at = jnp.where(filling, 0, t + 1)

        @pl.when(busy & (at < chunks))
        def _():
            unit(at, u)

        return carry

    lax.fori_loop(0, units + (chunks + 3) * slots, slot, 0)

    last = chunks - 1

    def drain(s, carry):
        ag1(last, steps - 1, s).wait_recv()
        for k in range(steps):
            rs1(last, k, s).wait_send()
            rs2(last, k, s).wait_send()
            ag2(last, k, s, k == 0).wait_send()
            ag1(last, k, s).wait_send()
        return carry

    lax.fori_loop(0, STREAMS, drain, 0)


def solution(mesh):
    tp = mesh.shape["tp"]
    side = math.isqrt(tp)

    def step(x, w_gate, w_up, w_down):
        rows, depth = x.shape
        ff, d_out = w_down.shape
        width = d_out // STREAMS
        piece = CHUNK // side
        sub = piece // side
        steps = side - 1
        any_spec = pl.BlockSpec(memory_space=pl.ANY)
        dma = pltpu.SemaphoreType.DMA
        return pl.pallas_call(
            functools.partial(kernel, side),
            out_shape=jax.ShapeDtypeStruct((rows, d_out), BF16),
            in_specs=[any_spec] * 4,
            out_specs=any_spec,
            scratch_shapes=[
                pltpu.VMEM((2, CHUNK, depth), BF16),
                pltpu.VMEM((GU_SLOTS, depth, 2 * TILE), BF16),
                pltpu.VMEM((DN_SLOTS, ff, width), BF16),
                pltpu.VMEM((ff // TILE, CHUNK, TILE), BF16),
                pltpu.VMEM((2, STREAMS, CHUNK, width), F32),
                pltpu.VMEM((2, STREAMS, piece, width), F32),
                pltpu.VMEM((steps, STREAMS, piece, width), BF16),
                pltpu.VMEM((2, steps, STREAMS, piece, width), BF16),
                pltpu.VMEM((steps, STREAMS, sub, width), BF16),
                pltpu.VMEM((2, steps, STREAMS, sub, width), BF16),
                pltpu.VMEM((STREAMS, sub, width), BF16),
                dma((2,)),
                dma((GU_SLOTS, 2)),
                dma((DN_SLOTS,)),
                dma((STREAMS,)),
            ]
            + [dma((steps, STREAMS)), dma((2, steps, STREAMS))] * 4,
            compiler_params=pltpu.CompilerParams(
                collective_id=0, has_side_effects=True, vmem_limit_bytes=66_000_000
            ),
            cost_estimate=pl.CostEstimate(
                flops=6 * rows * depth * ff, bytes_accessed=8 * 3 * depth * ff * 2, transcendentals=rows * ff
            ),
            name="mlp_ring",
        )(x, w_gate, w_up, w_down)

    return jax.shard_map(
        step,
        mesh=mesh,
        in_specs=(P("dp", None), P(None, "tp"), P(None, "tp"), P("tp", None)),
        out_specs=P("dp", None),
        check_vma=False,
    )
```

```python
import functools
import math

import jax
import jax.numpy as jnp
from jax import lax
from jax.experimental import pallas as pl
from jax.experimental.pallas import tpu as pltpu
from jax.sharding import PartitionSpec as P

F32 = jnp.float32
BF16 = jnp.bfloat16

CHUNK = 256
STREAMS = 8
TILE = 128
COPY_FLOPS = 4096
GU_SLOTS = 3
DN_SLOTS = 3


def kernel(
    side,
    x_hbm, wg_hbm, wu_hbm, wd_hbm, y_hbm,
    x_buf, gu_buf, dn_buf, hidden, part, xred, out1, in1, out2, in2, fin,
    x_sem, gu_sem, dn_sem, fin_sem,
    send1, recv1, send2, recv2, send3, recv3, send4, recv4,
):
    rows, depth = x_hbm.shape
    width = wd_hbm.shape[1] // STREAMS
    ff = wg_hbm.shape[1]
    chunks = rows // CHUNK
    piece = CHUNK // side
    sub = piece // side
    steps = side - 1
    gu_units = ff // TILE
    units = gu_units + STREAMS
    slots = steps * 8

    me = lax.axis_index("tp")
    px, py = me // side, me % side

    def place(stream):
        colour = stream % 4
        first_x = 1 - colour // 2
        d = 1 - 2 * (colour % 2)
        along_x = ((px + d + side) % side) * side + py
        along_y = px * side + (py + d + side) % side
        p1 = first_x * px + (1 - first_x) * py
        p2 = first_x * py + (1 - first_x) * px
        n1 = first_x * along_x + (1 - first_x) * along_y
        n2 = first_x * along_y + (1 - first_x) * along_x
        return d, p1, p2, n1, n2

    def cols(stream):
        slab = 2 * (stream % 4) + stream // 4
        return pl.ds(pl.multiple_of(slab * width, 128), width)

    def colour_cols(c):
        return pl.ds(pl.multiple_of(c * 2 * width, 128), 2 * width)

    def y_rows(start, size):
        return pl.ds(pl.multiple_of(start, 16), size)

    def x_copy(j):
        return pltpu.make_async_copy(
            x_hbm.at[pl.ds(pl.multiple_of(j * CHUNK, CHUNK), CHUNK)], x_buf.at[j % 2], x_sem.at[j % 2]
        )

    def gu_copies(g):
        src = pl.ds(pl.multiple_of((g % gu_units) * TILE, TILE), TILE)
        slot = g % GU_SLOTS
        return (
            pltpu.make_async_copy(wg_hbm.at[:, src], gu_buf.at[slot, :, pl.ds(0, TILE)], gu_sem.at[slot, 0]),
            pltpu.make_async_copy(wu_hbm.at[:, src], gu_buf.at[slot, :, pl.ds(TILE, TILE)], gu_sem.at[slot, 1]),
        )

    def dn_copy(g):
        slot = g % DN_SLOTS
        return pltpu.make_async_copy(wd_hbm.at[:, cols(g % STREAMS)], dn_buf.at[slot], dn_sem.at[slot])

    def unit(j, u):
        @pl.when(u < gu_units)
        def _():
            g = j * gu_units + u

            @pl.when(u == 0)
            def _():
                x_copy(j).wait()

            for c in gu_copies(g):
                c.wait()
            both = jnp.dot(x_buf[j % 2], gu_buf[g % GU_SLOTS], preferred_element_type=F32)
            gate, up = both[:, :TILE], both[:, TILE:]
            hidden[u] = (jax.nn.silu(gate) * up).astype(BF16)

            @pl.when(g + GU_SLOTS < chunks * gu_units)
            def _():
                for c in gu_copies(g + GU_SLOTS):
                    c.start()

            @pl.when((u == gu_units - 1) & (j + 2 < chunks))
            def _():
                x_copy(j + 2).start()

            @pl.when((j == 0) & (u == gu_units // 2))
            def _():
                for i in range(DN_SLOTS):
                    dn_copy(i).start()

            @pl.when((j == 0) & (u == gu_units - 1))
            def _():
                x_copy(1).start()

        @pl.when(u >= gu_units)
        def _():
            s = u - gu_units
            g = j * STREAMS + s
            dn_copy(g).wait()
            h = jnp.concatenate([hidden[i] for i in range(gu_units)], axis=1)
            part[j % 2, s] = jnp.dot(h, dn_buf[g % DN_SLOTS], preferred_element_type=F32)

            @pl.when(g + DN_SLOTS < chunks * STREAMS)
            def _():
                dn_copy(g + DN_SLOTS).start()

    def remote(src, dst, ssem, rsem, to):
        return pltpu.make_async_remote_copy(
            src_ref=src, dst_ref=dst, send_sem=ssem, recv_sem=rsem,
            device_id={"tp": to}, device_id_type=pl.DeviceIdType.MESH,
        )

    def rs1(j, k, s):
        _, _, _, n1, _ = place(s)
        return remote(out1.at[k, s], in1.at[j % 2, k, s], send1.at[k, s], recv1.at[j % 2, k, s], n1)

    def rs2(j, k, c):
        _, _, _, _, n2 = place(c)
        return remote(out2.at[k, c], in2.at[j % 2, k, c], send2.at[k, c], recv2.at[j % 2, k, c], n2)

    def ag2(j, k, c, own):
        d, p1, p2, _, n2 = place(c)
        r = (p2 - d * k + 2 * side) % side
        at = y_hbm.at[y_rows(j * CHUNK + p1 * piece + r * sub, sub), colour_cols(c)]
        return remote(fin.at[c] if own else at, at, send3.at[k, c], recv3.at[j % 2, k, c], n2)

    def ag1(j, k, s):
        d, p1, _, n1, _ = place(s)
        q = (p1 - d * k + 2 * side) % side
        at = y_hbm.at[y_rows(j * CHUNK + q * piece, piece), cols(s)]
        return remote(at, at, send4.at[k, s], recv4.at[j % 2, k, s], n1)

    def fin_copy(j, c):
        _, p1, p2, _, _ = place(c)
        at = y_hbm.at[y_rows(j * CHUNK + p1 * piece + p2 * sub, sub), colour_cols(c)]
        return pltpu.make_async_copy(fin.at[c], at, fin_sem.at[c])

    def each(first, count, f):
        lax.fori_loop(first, first + count, lambda s, _: (f(s), 0)[1], 0)

    def phase1(j, k, first, count):
        def add(s):
            d, p1, _, _, _ = place(s)
            q = (p1 - d * (1 + k) + 2 * side) % side
            mine = part[j % 2, s, pl.ds(pl.multiple_of(q * piece, piece), piece), :]

            @pl.when(j > 0)
            def _():
                rs1(j - 1, k, s).wait_send()

            @pl.when(k == 0)
            def _():
                out1[0, s] = mine.astype(BF16)

            @pl.when(k > 0)
            def _():
                rs1(j, k - 1, s).wait_recv()
                out1[k, s] = (mine + in1[j % 2, k - 1, s].astype(F32)).astype(BF16)

        each(first, count, add)
        each(first, count, lambda s: rs1(j, k, s).start())

    def phase2(j, k):
        def add(c):
            d, p1, p2, _, _ = place(c)
            r = (p2 - d * (1 + k) + 2 * side) % side
            at = pl.ds(pl.multiple_of(r * sub, sub), sub)

            @pl.when(j > 0)
            def _():
                rs2(j - 1, k, c).wait_send()

            @pl.when(k == 0)
            def _():
                for h in range(2):
                    s = 4 * h + c
                    rs1(j, steps - 1, s).wait_recv()
                    mine = part[j % 2, s, pl.ds(pl.multiple_of(p1 * piece, piece), piece), :]
                    xred[j % 2, s] = mine + in1[j % 2, steps - 1, s].astype(F32)
                    out2[0, c, h] = xred[j % 2, s, at, :].astype(BF16)

            @pl.when(k > 0)
            def _():
                rs2(j, k - 1, c).wait_recv()
                for h in range(2):
                    mine = xred[j % 2, 4 * h + c, at, :]
                    out2[k, c, h] = (mine + in2[j % 2, k - 1, c, h].astype(F32)).astype(BF16)

        each(0, 4, add)
        each(0, 4, lambda c: rs2(j, k, c).start())

    def phase3(j, k):
        @pl.when(k == 0)
        def _():
            def add(c):
                _, _, p2, _, _ = place(c)

                @pl.when(j > 0)
                def _():
                    ag2(j - 1, 0, c, True).wait_send()

                rs2(j, steps - 1, c).wait_recv()
                for h in range(2):
                    mine = xred[j % 2, 4 * h + c, pl.ds(pl.multiple_of(p2 * sub, sub), sub), :]
                    total = mine + in2[j % 2, steps - 1, c, h].astype(F32)
                    fin[c, :, h * width : (h + 1) * width] = total.astype(BF16)

            def go(c):
                ag2(j, 0, c, True).start()
                fin_copy(j, c).start()

            each(0, 4, add)
            each(0, 4, go)

        @pl.when(k > 0)
        def _():
            def go(c):
                @pl.when(j > 0)
                def _():
                    ag2(j - 1, k, c, False).wait_send()

                @pl.when(k == 1)
                def _():
                    fin_copy(j, c).wait()

                ag2(j, k - 1, c, False).wait_recv()
                ag2(j, k, c, False).start()

            each(0, 4, go)

    def phase4(j, k, half):
        def go(s):
            @pl.when(j > 0)
            def _():
                ag1(j - 1, k, s).wait_send()

            @pl.when(k == 0)
            def _():
                @pl.when(s < 4)
                def _():
                    ag2(j, steps - 1, s, False).wait_recv()

                @pl.when(j > 0)
                def _():
                    ag1(j - 1, steps - 1, s).wait_recv()

            @pl.when(k > 0)
            def _():
                ag1(j, k - 1, s).wait_recv()

            ag1(j, k, s).start()

        each(4 * half, 4, go)

    x_copy(0).start()
    for g in range(GU_SLOTS):
        for c in gu_copies(g):
            c.start()

    barrier = pltpu.get_barrier_semaphore()
    for to in (
        ((px + 1) % side) * side + py,
        ((px + side - 1) % side) * side + py,
        px * side + (py + 1) % side,
        px * side + (py + side - 1) % side,
    ):
        pl.semaphore_signal(barrier, inc=1, device_id={"tp": to}, device_id_type=pl.DeviceIdType.MESH)
    pl.semaphore_wait(barrier, 4)

    last = chunks - 1
    fill = units + 1

    def turn(n, carry):
        filling = n < fill
        i = jnp.where(filling, 0, n - fill)
        t, rest = i // slots, i % slots
        k, m = rest // 8, rest % 8
        half = m % 2

        ready = jnp.where(filling, n - 1 - gu_units, 4 * half)
        again = (n >= fill) & (m < 2) & (t < chunks) & ((t > 0) | (k > 0))

        @pl.when((filling & (n > gu_units)) | again)
        def _():
            phase1(t, k, ready, jnp.where(filling, 1, 4))

        @pl.when((n >= fill) & (m == 2) & (t >= 1) & (t - 1 < chunks))
        def _():
            phase2(t - 1, k)

        @pl.when((n >= fill) & (m == 4) & (t >= 2) & (t - 2 < chunks))
        def _():
            phase3(t - 2, k)

        @pl.when((n >= fill) & (m >= 6) & (t >= 3) & (t - 3 < last))
        def _():
            phase4(t - 3, k, half)

        u = jnp.where(filling, n, (units * rest) // slots)
        busy = (n < units) | ((n >= fill) & ((units * (rest + 1)) // slots > (units * rest) // slots))
        at = jnp.where(filling, 0, t + 1)

        @pl.when(busy & (at < chunks))
        def _():
            unit(at, u)

        return carry

    lax.fori_loop(0, fill + (chunks + 2) * slots, turn, 0)

    def drain(s, carry):
        ag1(last - 1, steps - 1, s).wait_recv()
        for k in range(steps):
            rs1(last, k, s).wait_send()
            ag1(last - 1, k, s).wait_send()
        return carry

    def drain2(c, carry):
        ag2(last, steps - 1, c, False).wait_recv()
        for k in range(steps):
            rs2(last, k, c).wait_send()
            ag2(last, k, c, k == 0).wait_send()
        return carry

    lax.fori_loop(0, STREAMS, drain, 0)
    lax.fori_loop(0, 4, drain2, 0)


def copy_rows(src_ref, *refs):
    refs[-1][...] = src_ref[...]


def copy_into(src, dst, first, count, block):
    rows, width = src.shape
    at = first // block
    spec = pl.BlockSpec((block, width), lambda i: (i + at, 0))
    return pl.pallas_call(
        copy_rows,
        grid=(count // block,),
        out_shape=jax.ShapeDtypeStruct(src.shape, src.dtype),
        in_specs=[spec] + ([] if dst is None else [pl.BlockSpec(memory_space=pl.ANY)]),
        out_specs=spec,
        input_output_aliases={} if dst is None else {1: 0},
        compiler_params=pltpu.CompilerParams(vmem_limit_bytes=44 << 20),
        cost_estimate=pl.CostEstimate(
            flops=count * width * COPY_FLOPS, bytes_accessed=4 * count * width, transcendentals=0
        ),
        name="copy_rows",
    )(*([src] if dst is None else [src, dst]))


def place_pieces(side, n_in, base, *refs):
    ins, out, sems = refs[:n_in], refs[n_in + 1], refs[n_in + 2]
    me = lax.axis_index("tp")
    px, py = me // side, me % side
    piece = ins[0].shape[0]
    half, quarter = ins[0].shape[1], ins[0].shape[1] // 2
    stores = []
    for axis, p in enumerate((px, py)):
        for n, (shift, col, w) in enumerate(
            ((0, 0, half), (side - 1, 0, half), (1, 0, half), (side - 2, 0, quarter), (2, quarter, quarter))
        ):
            i = axis * 5 + n
            at = pl.ds(pl.multiple_of(base + (p + shift) % side * piece, piece), piece)
            stores.append(
                pltpu.make_async_copy(ins[i], out.at[at, pl.ds(axis * half + col, w)], sems.at[i])
            )
    for store in stores:
        store.start()
    for store in stores:
        store.wait()


def finish(side, y, base, pieces):
    n = len(pieces)
    any_spec = pl.BlockSpec(memory_space=pl.ANY)
    return pl.pallas_call(
        functools.partial(place_pieces, side, n, base),
        out_shape=jax.ShapeDtypeStruct(y.shape, y.dtype),
        in_specs=[pl.BlockSpec(memory_space=pltpu.VMEM)] * n + [any_spec],
        out_specs=any_spec,
        scratch_shapes=[pltpu.SemaphoreType.DMA((n,))],
        input_output_aliases={n: 0},
        compiler_params=pltpu.CompilerParams(vmem_limit_bytes=8 << 20),
        name="place_pieces",
    )(*pieces, y)


def gather_last(side, y):
    rows, d_out = y.shape
    half, quarter, piece, base = d_out // 2, d_out // 4, CHUNK // side, rows - CHUNK
    me = lax.axis_index("tp")
    px, py = me // side, me % side

    def ring(dx, dy):
        grid = [(x, w) for x in range(side) for w in range(side)]
        return [(x * side + w, (x + dx) % side * side + (w + dy) % side) for x, w in grid]

    pieces = []
    near, own = [], []
    for axis, p in enumerate((px, py)):
        mine = lax.dynamic_slice(y, (base + p * piece, axis * half), (piece, half))
        own.append(mine)
    for axis in range(2):
        step = (1, 0) if axis == 0 else (0, 1)
        back = (-1, 0) if axis == 0 else (0, -1)
        near.append((lax.ppermute(own[axis], "tp", ring(*step)), lax.ppermute(own[axis], "tp", ring(*back))))
    part = base * 5 // 8 // 128 * 128
    out = copy_into(y, None, 0, part, 128)
    (near, out) = lax.optimization_barrier((near, out))
    far = []
    for axis in range(2):
        step = (1, 0) if axis == 0 else (0, 1)
        back = (-1, 0) if axis == 0 else (0, -1)
        from_back, from_ahead = near[axis]
        far.append(
            (
                lax.ppermute(from_back[:, :quarter], "tp", ring(*step)),
                lax.ppermute(from_ahead[:, quarter:], "tp", ring(*back)),
            )
        )
    out = copy_into(y, out, part, base - part, 128)
    for axis in range(2):
        pieces += [own[axis], *near[axis], *far[axis]]
    return finish(side, out, base, pieces)


def solution(mesh):
    tp = mesh.shape["tp"]
    side = math.isqrt(tp)

    def step(x, w_gate, w_up, w_down):
        rows, depth = x.shape
        ff, d_out = w_down.shape
        width = d_out // STREAMS
        piece = CHUNK // side
        sub = piece // side
        steps = side - 1
        any_spec = pl.BlockSpec(memory_space=pl.ANY)
        dma = pltpu.SemaphoreType.DMA
        y = pl.pallas_call(
            functools.partial(kernel, side),
            out_shape=jax.ShapeDtypeStruct((rows, d_out), BF16),
            in_specs=[any_spec] * 4,
            out_specs=any_spec,
            scratch_shapes=[
                pltpu.VMEM((2, CHUNK, depth), BF16),
                pltpu.VMEM((GU_SLOTS, depth, 2 * TILE), BF16),
                pltpu.VMEM((DN_SLOTS, ff, width), BF16),
                pltpu.VMEM((ff // TILE, CHUNK, TILE), BF16),
                pltpu.VMEM((2, STREAMS, CHUNK, width), F32),
                pltpu.VMEM((2, STREAMS, piece, width), F32),
                pltpu.VMEM((steps, STREAMS, piece, width), BF16),
                pltpu.VMEM((2, steps, STREAMS, piece, width), BF16),
                pltpu.VMEM((steps, 4, 2, sub, width), BF16),
                pltpu.VMEM((2, steps, 4, 2, sub, width), BF16),
                pltpu.VMEM((4, sub, 2 * width), BF16),
                dma((2,)),
                dma((GU_SLOTS, 2)),
                dma((DN_SLOTS,)),
                dma((4,)),
            ]
            + [dma((steps, n)) if one else dma((2, steps, n)) for n in (8, 4, 4, 8) for one in (1, 0)],
            compiler_params=pltpu.CompilerParams(
                collective_id=0, has_side_effects=True, vmem_limit_bytes=66_000_000
            ),
            cost_estimate=pl.CostEstimate(
                flops=6 * rows * depth * ff, bytes_accessed=8 * 3 * depth * ff * 2, transcendentals=rows * ff
            ),
            name="mlp_ring",
        )(x, w_gate, w_up, w_down)
        return gather_last(side, y)

    return jax.shard_map(
        step,
        mesh=mesh,
        in_specs=(P("dp", None), P(None, "tp"), P(None, "tp"), P("tp", None)),
        out_specs=P("dp", None),
        check_vma=False,
    )
```

```python
import functools
import math

import jax
import jax.numpy as jnp
from jax import lax
from jax.experimental import pallas as pl
from jax.experimental.pallas import tpu as pltpu
from jax.sharding import PartitionSpec as P

F32 = jnp.float32
BF16 = jnp.bfloat16

CHUNK = 256
STREAMS = 8
TILE = 128
COPY_ROWS = 128
LOW_CHUNKS = 4
LIMIT = 20 << 20
GU_SLOTS = 3
DN_SLOTS = 3


def kernel(
    side,
    x_hbm, wg_hbm, wu_hbm, wd_hbm, y_hbm, y_vmem,
    x_buf, gu_buf, dn_buf, hidden, part, xred, out1, in1, out2, in2, fin,
    x_sem, gu_sem, dn_sem, fin_sem,
    send1, recv1, send2, recv2, send3, recv3, send4, recv4,
):
    rows, depth = x_hbm.shape
    width = wd_hbm.shape[1] // STREAMS
    ff = wg_hbm.shape[1]
    chunks = rows // CHUNK
    piece = CHUNK // side
    sub = piece // side
    steps = side - 1
    gu_units = ff // TILE
    units = gu_units + STREAMS
    slots = steps * 8

    me = lax.axis_index("tp")
    px, py = me // side, me % side

    def place(stream):
        colour = stream % 4
        first_x = 1 - colour // 2
        d = 1 - 2 * (colour % 2)
        along_x = ((px + d + side) % side) * side + py
        along_y = px * side + (py + d + side) % side
        p1 = first_x * px + (1 - first_x) * py
        p2 = first_x * py + (1 - first_x) * px
        n1 = first_x * along_x + (1 - first_x) * along_y
        n2 = first_x * along_y + (1 - first_x) * along_x
        return d, p1, p2, n1, n2

    def cols(stream):
        slab = 2 * (stream % 4) + stream // 4
        return pl.ds(pl.multiple_of(slab * width, 128), width)

    def colour_cols(c):
        return pl.ds(pl.multiple_of(c * 2 * width, 128), 2 * width)

    def y_rows(start, size):
        return pl.ds(pl.multiple_of(start, 16), size)

    high = chunks - LOW_CHUNKS

    def placed(j, f):
        @pl.when(j < high)
        def _():
            f(y_hbm, j * CHUNK)

        @pl.when(j >= high)
        def _():
            f(y_vmem, (j - high) * CHUNK)

    def x_copy(j):
        return pltpu.make_async_copy(
            x_hbm.at[pl.ds(pl.multiple_of(j * CHUNK, CHUNK), CHUNK)], x_buf, x_sem
        )

    def gu_copies(g):
        src = pl.ds(pl.multiple_of((g % gu_units) * TILE, TILE), TILE)
        slot = g % GU_SLOTS
        return (
            pltpu.make_async_copy(wg_hbm.at[:, src], gu_buf.at[slot, :, pl.ds(0, TILE)], gu_sem.at[slot, 0]),
            pltpu.make_async_copy(wu_hbm.at[:, src], gu_buf.at[slot, :, pl.ds(TILE, TILE)], gu_sem.at[slot, 1]),
        )

    def dn_copy(g):
        slot = g % DN_SLOTS
        return pltpu.make_async_copy(wd_hbm.at[:, cols(g % STREAMS)], dn_buf.at[slot], dn_sem.at[slot])

    def unit(j, u):
        @pl.when(u < gu_units)
        def _():
            g = j * gu_units + u

            @pl.when(u == 0)
            def _():
                x_copy(j).wait()

            for c in gu_copies(g):
                c.wait()
            both = jnp.dot(x_buf[...], gu_buf[g % GU_SLOTS], preferred_element_type=F32)
            gate, up = both[:, :TILE], both[:, TILE:]
            hidden[u] = (jax.nn.silu(gate) * up).astype(BF16)

            @pl.when(g + GU_SLOTS < chunks * gu_units)
            def _():
                for c in gu_copies(g + GU_SLOTS):
                    c.start()

            @pl.when((u == gu_units - 1) & (j + 1 < chunks))
            def _():
                x_copy(j + 1).start()

            @pl.when((j == 0) & (u == gu_units // 2))
            def _():
                for i in range(DN_SLOTS):
                    dn_copy(i).start()

        @pl.when(u >= gu_units)
        def _():
            s = u - gu_units
            g = j * STREAMS + s
            dn_copy(g).wait()
            h = jnp.concatenate([hidden[i] for i in range(gu_units)], axis=1)
            part[j % 2, s] = jnp.dot(h, dn_buf[g % DN_SLOTS], preferred_element_type=F32)

            @pl.when(g + DN_SLOTS < chunks * STREAMS)
            def _():
                dn_copy(g + DN_SLOTS).start()

    def remote(src, dst, ssem, rsem, to):
        return pltpu.make_async_remote_copy(
            src_ref=src, dst_ref=dst, send_sem=ssem, recv_sem=rsem,
            device_id={"tp": to}, device_id_type=pl.DeviceIdType.MESH,
        )

    def rs1(j, k, s):
        _, _, _, n1, _ = place(s)
        return remote(out1.at[k, s], in1.at[j % 2, k, s], send1.at[k, s], recv1.at[j % 2, k, s], n1)

    def rs2(j, k, c):
        _, _, _, _, n2 = place(c)
        return remote(out2.at[k, c], in2.at[j % 2, k, c], send2.at[k, c], recv2.at[j % 2, k, c], n2)

    def ag2(j, k, c, own, y=y_hbm, row=0):
        d, p1, p2, _, n2 = place(c)
        r = (p2 - d * k + 2 * side) % side
        at = y.at[y_rows(row + p1 * piece + r * sub, sub), colour_cols(c)]
        return remote(fin.at[c] if own else at, at, send3.at[k, c], recv3.at[j % 2, k, c], n2)

    def ag1(j, k, s, y=y_hbm, row=0):
        d, p1, _, n1, _ = place(s)
        q = (p1 - d * k + 2 * side) % side
        at = y.at[y_rows(row + q * piece, piece), cols(s)]
        return remote(at, at, send4.at[k, s], recv4.at[j % 2, k, s], n1)

    def fin_copy(c, y, row):
        _, p1, p2, _, _ = place(c)
        at = y.at[y_rows(row + p1 * piece + p2 * sub, sub), colour_cols(c)]
        return pltpu.make_async_copy(fin.at[c], at, fin_sem.at[c])

    def each(first, count, f):
        lax.fori_loop(first, first + count, lambda s, _: (f(s), 0)[1], 0)

    def phase1(j, k, first, count):
        def add(s):
            d, p1, _, _, _ = place(s)
            q = (p1 - d * (1 + k) + 2 * side) % side
            mine = part[j % 2, s, pl.ds(pl.multiple_of(q * piece, piece), piece), :]

            @pl.when(j > 0)
            def _():
                rs1(j - 1, k, s).wait_send()

            @pl.when(k == 0)
            def _():
                out1[0, s] = mine.astype(BF16)

            @pl.when(k > 0)
            def _():
                rs1(j, k - 1, s).wait_recv()
                out1[k, s] = (mine + in1[j % 2, k - 1, s].astype(F32)).astype(BF16)

        each(first, count, add)
        each(first, count, lambda s: rs1(j, k, s).start())

    def phase2(j, k):
        def add(c):
            d, p1, p2, _, _ = place(c)
            r = (p2 - d * (1 + k) + 2 * side) % side
            at = pl.ds(pl.multiple_of(r * sub, sub), sub)

            @pl.when(j > 0)
            def _():
                rs2(j - 1, k, c).wait_send()

            @pl.when(k == 0)
            def _():
                for h in range(2):
                    s = 4 * h + c
                    rs1(j, steps - 1, s).wait_recv()
                    mine = part[j % 2, s, pl.ds(pl.multiple_of(p1 * piece, piece), piece), :]
                    xred[j % 2, s] = mine + in1[j % 2, steps - 1, s].astype(F32)
                    out2[0, c, h] = xred[j % 2, s, at, :].astype(BF16)

            @pl.when(k > 0)
            def _():
                rs2(j, k - 1, c).wait_recv()
                for h in range(2):
                    mine = xred[j % 2, 4 * h + c, at, :]
                    out2[k, c, h] = (mine + in2[j % 2, k - 1, c, h].astype(F32)).astype(BF16)

        each(0, 4, add)
        each(0, 4, lambda c: rs2(j, k, c).start())

    def phase3(j, k):
        @pl.when(k == 0)
        def _():
            def add(c):
                _, p1, p2, _, _ = place(c)

                @pl.when(j > 0)
                def _():
                    ag2(j - 1, 0, c, True).wait_send()

                rs2(j, steps - 1, c).wait_recv()
                for h in range(2):
                    mine = xred[j % 2, 4 * h + c, pl.ds(pl.multiple_of(p2 * sub, sub), sub), :]
                    total = (mine + in2[j % 2, steps - 1, c, h].astype(F32)).astype(BF16)
                    fin[c, :, h * width : (h + 1) * width] = total

                    @pl.when(j >= high)
                    def _():
                        at = y_rows((j - high) * CHUNK + p1 * piece + p2 * sub, sub)
                        y_vmem[at, pl.ds(pl.multiple_of((2 * c + h) * width, 128), width)] = total

            def go(c):
                placed(j, lambda y, row: ag2(j, 0, c, True, y, row).start())

                @pl.when(j < high)
                def _():
                    fin_copy(c, y_hbm, j * CHUNK).start()

            each(0, 4, add)
            each(0, 4, go)

        @pl.when(k > 0)
        def _():
            def go(c):
                @pl.when(j > 0)
                def _():
                    ag2(j - 1, k, c, False).wait_send()

                @pl.when((k == 1) & (j < high))
                def _():
                    fin_copy(c, y_hbm, j * CHUNK).wait()

                ag2(j, k - 1, c, False).wait_recv()
                placed(j, lambda y, row: ag2(j, k, c, False, y, row).start())

            each(0, 4, go)

    def phase4(j, k, half):
        def go(s):
            @pl.when(j > 0)
            def _():
                ag1(j - 1, k, s).wait_send()

            @pl.when(k == 0)
            def _():
                @pl.when(s < 4)
                def _():
                    ag2(j, steps - 1, s, False).wait_recv()

                @pl.when(j > 0)
                def _():
                    ag1(j - 1, steps - 1, s).wait_recv()

            @pl.when(k > 0)
            def _():
                ag1(j, k - 1, s).wait_recv()

            placed(j, lambda y, row: ag1(j, k, s, y, row).start())

        each(4 * half, 4, go)

    x_copy(0).start()
    for g in range(GU_SLOTS):
        for c in gu_copies(g):
            c.start()

    barrier = pltpu.get_barrier_semaphore()
    for to in (
        ((px + 1) % side) * side + py,
        ((px + side - 1) % side) * side + py,
        px * side + (py + 1) % side,
        px * side + (py + side - 1) % side,
    ):
        pl.semaphore_signal(barrier, inc=1, device_id={"tp": to}, device_id_type=pl.DeviceIdType.MESH)
    pl.semaphore_wait(barrier, 4)

    last = chunks - 1
    fill = units + 1

    def turn(n, carry):
        filling = n < fill
        i = jnp.where(filling, 0, n - fill)
        t, rest = i // slots, i % slots
        k, m = rest // 8, rest % 8
        half = m % 2

        ready = jnp.where(filling, n - 1 - gu_units, 4 * half)
        again = (n >= fill) & (m < 2) & (t < chunks) & ((t > 0) | (k > 0))

        @pl.when((filling & (n > gu_units)) | again)
        def _():
            phase1(t, k, ready, jnp.where(filling, 1, 4))

        @pl.when((n >= fill) & (m == 2) & (t >= 1) & (t - 1 < chunks))
        def _():
            phase2(t - 1, k)

        @pl.when((n >= fill) & (m == 4) & (t >= 2) & (t - 2 < chunks))
        def _():
            phase3(t - 2, k)

        @pl.when((n >= fill) & (m >= 6) & (t >= 3))
        def _():
            phase4(t - 3, k, half)

        u = jnp.where(filling, n, (units * rest) // slots)
        busy = (n < units) | ((n >= fill) & ((units * (rest + 1)) // slots > (units * rest) // slots))
        at = jnp.where(filling, 0, t + 1)

        @pl.when(busy & (at < chunks))
        def _():
            unit(at, u)

        return carry

    lax.fori_loop(0, fill + (chunks + 3) * slots, turn, 0)

    def drain(s, carry):
        ag1(last, steps - 1, s).wait_recv()
        for k in range(steps):
            rs1(last, k, s).wait_send()
            ag1(last, k, s).wait_send()
        return carry

    def drain2(c, carry):
        for k in range(steps):
            rs2(last, k, c).wait_send()
            ag2(last, k, c, k == 0).wait_send()
        return carry

    lax.fori_loop(0, STREAMS, drain, 0)
    lax.fori_loop(0, 4, drain2, 0)


def copy_kernel(high_ref, low_ref, out_ref, buf, load_sem, store_sem, direct_sem):
    rows_low = low_ref.shape[0]
    rows_high = high_ref.shape[0] - rows_low
    n = rows_high // COPY_ROWS
    slots = buf.shape[0]

    def load(i):
        return pltpu.make_async_copy(high_ref.at[pl.ds(i * COPY_ROWS, COPY_ROWS)], buf.at[i % slots], load_sem.at[i % slots])

    def store(i):
        return pltpu.make_async_copy(buf.at[i % slots], out_ref.at[pl.ds(i * COPY_ROWS, COPY_ROWS)], store_sem.at[i % slots])

    pieces = rows_low // COPY_ROWS
    direct = [
        pltpu.make_async_copy(
            low_ref.at[pl.ds(i * COPY_ROWS, COPY_ROWS)],
            out_ref.at[pl.ds(rows_high + i * COPY_ROWS, COPY_ROWS)],
            direct_sem.at[i],
        )
        for i in range(pieces)
    ]
    for i in range(min(slots, n)):
        load(i).start()
    for c in direct:
        c.start()
    for i in range(n):
        load(i).wait()
        store(i).start()
        if i + slots < n:
            store(i).wait()
            load(i + slots).start()
    for i in range(max(n - slots, 0), n):
        store(i).wait()
    for c in direct:
        c.wait()


def join(high, low):
    rows, d_out = high.shape
    slots = min(6, (rows - low.shape[0]) // COPY_ROWS)
    return pl.pallas_call(
        copy_kernel,
        out_shape=jax.ShapeDtypeStruct((rows, d_out), BF16),
        in_specs=[pl.BlockSpec(memory_space=pl.ANY), pl.BlockSpec(memory_space=pltpu.VMEM)],
        out_specs=pl.BlockSpec(memory_space=pl.ANY),
        scratch_shapes=[
            pltpu.VMEM((slots, COPY_ROWS, d_out), BF16),
            pltpu.SemaphoreType.DMA((slots,)),
            pltpu.SemaphoreType.DMA((slots,)),
            pltpu.SemaphoreType.DMA((low.shape[0] // COPY_ROWS,)),
        ],
        compiler_params=pltpu.CompilerParams(vmem_limit_bytes=LIMIT),
        name="join",
    )(high, low)


def solution(mesh):
    tp = mesh.shape["tp"]
    side = math.isqrt(tp)

    def step(x, w_gate, w_up, w_down):
        rows, depth = x.shape
        ff, d_out = w_down.shape
        width = d_out // STREAMS
        piece = CHUNK // side
        sub = piece // side
        steps = side - 1
        low = LOW_CHUNKS * CHUNK
        any_spec = pl.BlockSpec(memory_space=pl.ANY)
        dma = pltpu.SemaphoreType.DMA
        y = pl.pallas_call(
            functools.partial(kernel, side),
            out_shape=(
                jax.ShapeDtypeStruct((rows, d_out), BF16),
                pltpu.VMEM((low, d_out), BF16),
            ),
            in_specs=[any_spec] * 4,
            out_specs=(any_spec, pl.BlockSpec(memory_space=pltpu.VMEM)),
            scratch_shapes=[
                pltpu.VMEM((CHUNK, depth), BF16),
                pltpu.VMEM((GU_SLOTS, depth, 2 * TILE), BF16),
                pltpu.VMEM((DN_SLOTS, ff, width), BF16),
                pltpu.VMEM((ff // TILE, CHUNK, TILE), BF16),
                pltpu.VMEM((2, STREAMS, CHUNK, width), F32),
                pltpu.VMEM((2, STREAMS, piece, width), F32),
                pltpu.VMEM((steps, STREAMS, piece, width), BF16),
                pltpu.VMEM((2, steps, STREAMS, piece, width), BF16),
                pltpu.VMEM((steps, 4, 2, sub, width), BF16),
                pltpu.VMEM((2, steps, 4, 2, sub, width), BF16),
                pltpu.VMEM((4, sub, 2 * width), BF16),
                dma,
                dma((GU_SLOTS, 2)),
                dma((DN_SLOTS,)),
                dma((4,)),
            ]
            + [dma((steps, n)) if one else dma((2, steps, n)) for n in (8, 4, 4, 8) for one in (1, 0)],
            compiler_params=pltpu.CompilerParams(
                collective_id=0, has_side_effects=True, vmem_limit_bytes=51_900_000
            ),
            cost_estimate=pl.CostEstimate(
                flops=6 * rows * depth * ff, bytes_accessed=8 * 3 * depth * ff * 2, transcendentals=rows * ff
            ),
            name="mlp_ring",
        )(x, w_gate, w_up, w_down)
        return join(*y)

    return jax.shard_map(
        step,
        mesh=mesh,
        in_specs=(P("dp", None), P(None, "tp"), P(None, "tp"), P("tp", None)),
        out_specs=P("dp", None),
        check_vma=False,
    )
```
